32 devices in a mesh: blk: 16 (over z, y, core), tensor: 2 (over x).
Axes of the slice: x: 2, y: 2, z: 4, core: 2. Of those that a mesh axis runs over, the one named last changes fastest.
Arguments:
- tokens: bfloat16 [64, 8192], P('blk'), may hold values from -6 to 6
- gate_weight: bfloat16 [29568, 8192], P(('blk', 'tensor')), may hold values from -0.0625 to 0.0625
- up_weight: bfloat16 [29568, 8192], P(('blk', 'tensor')), may hold values from -0.0625 to 0.0625
- down_weight: bfloat16 [29568, 8192], P(('blk', 'tensor')), may hold values from -0.03125 to 0.03125
Outputs:
- mixed: bfloat16 [64, 8192], P(('blk', 'tensor'))
The draws below stay inside these ranges and needn't reach their ends.
All inputs are finite; a program needn't handle non-finite values.
Results may differ from the reference program's by a relative error of at most 0.009.
Values may be sent and summed in bfloat16 or wider, within the bound.
A program may use at most 128 MiB of HBM per device.

```python
import jax
import jax.numpy as jnp

D = 8192
FF = 29568
TOKENS = 64


def level_of(own_key, extent, shards, low, high):
    factor_of, own = 1.0, jax.random.fold_in(own_key, 6)
    for axis_at, shards_of in shards:
        draws = jnp.exp(jax.random.uniform(jax.random.fold_in(own, axis_at), (shards_of,), jnp.float32, low / len(shards), high / len(shards)))
        factor_of = factor_of * jnp.repeat(draws, extent[axis_at] // shards_of).reshape([-1 if axis == axis_at else 1 for axis in range(len(extent))])
    return factor_of


def bell_draw(own_key, extent, width, most, pieces=(), kind=jnp.bfloat16):
    level = level_of(own_key, extent, pieces, -0.22, 0.18) if pieces else 1.0
    result = jax.random.normal(own_key, extent, jnp.float32) * width * level
    return jnp.minimum(jnp.maximum(result, -most), most).astype(kind)


def setup_inputs(seed: int = 0) -> dict:
    key_of = jax.random.split(jax.random.key(seed), 5)
    tokens = bell_draw(key_of[0], (TOKENS, D), 1.0, 6.0, ((0, 16),))
    gate_weight = bell_draw(key_of[1], (FF, D), D ** -0.5, 0.0625, ((0, 32),))
    up_weight = bell_draw(key_of[2], (FF, D), D ** -0.5, 0.0625, ((0, 32),))
    down_weight = bell_draw(key_of[3], (FF, D), FF ** -0.5, 0.03125, ((0, 32),))
    return {"tokens": tokens, "gate_weight": gate_weight, "up_weight": up_weight, "down_weight": down_weight}


def reference(tokens, gate_weight, up_weight, down_weight):
    gate = jnp.dot(tokens, gate_weight.T, preferred_element_type=jnp.float32)
    up = jnp.dot(tokens, up_weight.T, preferred_element_type=jnp.float32)
    hidden = (jax.nn.silu(gate) * up).astype(jnp.bfloat16)
    return jnp.dot(hidden, down_weight, preferred_element_type=jnp.float32).astype(jnp.bfloat16)
```

```python
import functools

import jax
import jax.numpy as jnp
from jax import lax
from jax.experimental import pallas as pl
from jax.experimental.pallas import tpu as pltpu
from jax.sharding import PartitionSpec as P

MESH = pl.DeviceIdType.MESH
CHUNKS = 4
TILE = 512


def kernel(
    chips, tensors,
    tok, wg, wu, wd, out,
    wgv, wuv, wdv, gathered, x2d, gacc, uacc, hid, own, part, near, stage, far,
    tok_sem, w_sem, ag_send, ag_recv, fw_send, fw_recv, near_send, near_recv, far_send, far_recv,
):
    blk, ten = lax.axis_index("blk"), lax.axis_index("tensor")
    core, chip = lax.rem(blk, 2), lax.div(blk, 2)
    other = 1 - core
    mate = (chip * 2 + other, ten)
    owners = chips * tensors
    me = chip * tensors + ten
    width = tok.shape[1] // CHUNKS
    rows = tok.shape[0]
    share = rows // tensors

    def owner_of(step):
        index = lax.rem(me + step, owners)
        return index, (lax.div(index, tensors) * 2 + core, lax.rem(index, tensors))

    def cols(k):
        return pl.ds(k * width, width)

    def tok_copy(k):
        return pltpu.make_async_copy(tok.at[:, cols(k)], gathered.at[k, core, chip], tok_sem.at[k])

    def w_copy(which, k):
        src, dst = ((wg, wgv), (wu, wuv), (wd, wdv))[which]
        return pltpu.make_async_copy(src.at[:, cols(k)], dst.at[k], w_sem.at[which, k])

    for k in range(CHUNKS):
        tok_copy(k).start()
    for k in range(CHUNKS):
        w_copy(0, k).start()
        w_copy(1, k).start()

    barrier = pltpu.get_barrier_semaphore()
    pl.semaphore_signal(barrier, inc=1, device_id=mate, device_id_type=MESH)

    @pl.loop(1, owners)
    def _(step):
        pl.semaphore_signal(barrier, inc=1, device_id=owner_of(step)[1], device_id_type=MESH)

    pl.semaphore_wait(barrier, owners)

    def ag_copy(k, step, slot):
        to = lax.rem(chip + step, chips)
        return pltpu.make_async_remote_copy(
            src_ref=gathered.at[k, core, slot], dst_ref=gathered.at[k, core, slot],
            send_sem=ag_send.at[k, to], recv_sem=ag_recv.at[k, slot],
            device_id=(to * 2 + core, ten), device_id_type=MESH,
        )

    def fw_copy(k, side):
        return pltpu.make_async_remote_copy(
            src_ref=gathered.at[k, side], dst_ref=gathered.at[k, side],
            send_sem=fw_send.at[k], recv_sem=fw_recv.at[k],
            device_id=mate, device_id_type=MESH,
        )

    for k in range(CHUNKS):
        tok_copy(k).wait()

        @pl.loop(1, chips)
        def _(step):
            ag_copy(k, step, chip).start()

    for k in range(CHUNKS):
        w_copy(2, k).start()

    def forward(k):
        @pl.loop(1, chips)
        def _(step):
            ag_copy(k, step, lax.rem(chip + step, chips)).wait_recv()

        fw_copy(k, core).start()

    gacc[...] = jnp.zeros_like(gacc)
    uacc[...] = jnp.zeros_like(uacc)

    def project(k, start, stop):
        @pl.loop(start, stop)
        def _(step):
            at = pl.ds(pl.multiple_of(step * TILE, TILE), TILE)
            for side in range(2):
                for c in range(chips):
                    low = (side * chips + c) * rows
                    x2d[low:low + rows, :] = gathered[k, side, c, :, at]
            x = x2d[...]
            dims = (((1,), (1,)), ((), ()))
            gacc[...] += lax.dot_general(x, wgv[k, :, at], dims, preferred_element_type=jnp.float32)
            uacc[...] += lax.dot_general(x, wuv[k, :, at], dims, preferred_element_type=jnp.float32)

    tiles = width // TILE
    forward(0)
    for k in range(CHUNKS):
        fw_copy(k, other).wait_recv()
        w_copy(0, k).wait()
        w_copy(1, k).wait()
        project(k, 0, tiles // 2)
        if k + 1 < CHUNKS:
            forward(k + 1)
        project(k, tiles // 2, tiles)

    gate = gacc[...]
    hid[...] = (gate / (1.0 + jnp.exp(-gate)) * uacc[...]).astype(hid.dtype)

    def near_copy(j):
        return pltpu.make_async_remote_copy(
            src_ref=part.at[j, other], dst_ref=near.at[j],
            send_sem=near_send.at[j], recv_sem=near_recv.at[j],
            device_id=mate, device_id_type=MESH,
        )

    def far_copy(j, step, slot):
        to, device = owner_of(step)
        return pltpu.make_async_remote_copy(
            src_ref=stage.at[j, to], dst_ref=far.at[j, slot],
            send_sem=far_send.at[j, to], recv_sem=far_recv.at[j, slot],
            device_id=device, device_id_type=MESH,
        )

    half = chips * rows

    def down(j):
        w_copy(2, j).wait()

        @pl.loop(0, tiles)
        def _(step):
            at = pl.ds(pl.multiple_of(step * TILE, TILE), TILE)
            p = jnp.dot(hid[...], wdv[j, :, at], preferred_element_type=jnp.float32)
            for side in range(2):
                piece = p[side * half:(side + 1) * half]
                own[j, side, :, at] = piece
                part[j, side, :, at] = piece.astype(part.dtype)

        near_copy(j).start()

    def send_far(j):
        near_copy(j).wait_recv()

        @pl.loop(0, tiles)
        def _(step):
            at = pl.ds(pl.multiple_of(step * TILE, TILE), TILE)
            s = own[j, core, :, at] + near[j, :, at].astype(jnp.float32)
            for d in range(owners):
                stage[j, d, :, at] = s[d * share:(d + 1) * share].astype(stage.dtype)

        @pl.loop(1, owners)
        def _(step):
            far_copy(j, step, me).start()

    for j in range(CHUNKS):
        down(j)
        if j:
            send_far(j - 1)
    send_far(CHUNKS - 1)

    for j in range(CHUNKS):
        @pl.loop(1, owners)
        def _(step):
            far_copy(j, step, lax.rem(me + step, owners)).wait_recv()

        def add(step, acc):
            return acc + far[j, lax.rem(me + step, owners)].astype(jnp.float32)

        total = lax.fori_loop(1, owners, add, stage[j, me].astype(jnp.float32))
        out[:, j * width:(j + 1) * width] = total.astype(out.dtype)

    for k in range(CHUNKS):
        @pl.loop(1, chips)
        def _(step):
            ag_copy(k, step, chip).wait_send()

        @pl.loop(1, owners)
        def _(step):
            far_copy(k, step, me).wait_send()

        fw_copy(k, core).wait_send()
        near_copy(k).wait_send()


def per_device(blks, tensors, tokens, gate_weight, up_weight, down_weight):
    rows, depth = tokens.shape
    units = gate_weight.shape[0]
    chips, width = blks // 2, depth // CHUNKS
    owners, share = chips * tensors, rows // tensors
    everyone, half = blks * rows, chips * rows
    bf, f32, dma = jnp.bfloat16, jnp.float32, pltpu.SemaphoreType.DMA
    anywhere = pl.BlockSpec(memory_space=pl.ANY)
    return pl.pallas_call(
        functools.partial(kernel, chips, tensors),
        out_shape=jax.ShapeDtypeStruct((share, depth), bf),
        in_specs=[anywhere] * 4,
        out_specs=pl.BlockSpec(memory_space=pltpu.VMEM),
        scratch_shapes=[
            pltpu.VMEM((CHUNKS, units, width), bf),
            pltpu.VMEM((CHUNKS, units, width), bf),
            pltpu.VMEM((CHUNKS, units, width), bf),
            pltpu.VMEM((CHUNKS, 2, chips, rows, width), bf),
            pltpu.VMEM((everyone, TILE), bf),
            pltpu.VMEM((everyone, units), f32),
            pltpu.VMEM((everyone, units), f32),
            pltpu.VMEM((everyone, units), bf),
            pltpu.VMEM((CHUNKS, 2, half, width), f32),
            pltpu.VMEM((CHUNKS, 2, half, width), bf),
            pltpu.VMEM((CHUNKS, half, width), bf),
            pltpu.VMEM((CHUNKS, owners, share, width), bf),
            pltpu.VMEM((CHUNKS, owners, share, width), bf),
            dma((CHUNKS,)),
            dma((3, CHUNKS)),
            dma((CHUNKS, chips)),
            dma((CHUNKS, chips)),
            dma((CHUNKS,)),
            dma((CHUNKS,)),
            dma((CHUNKS,)),
            dma((CHUNKS,)),
            dma((CHUNKS, owners)),
            dma((CHUNKS, owners)),
        ],
        compiler_params=pltpu.CompilerParams(
            collective_id=0, has_side_effects=True, vmem_limit_bytes=60 * 1024 * 1024
        ),
    )(tokens, gate_weight, up_weight, down_weight)


def solution(mesh):
    placed = (
        P("blk", None),
        P(("blk", "tensor"), None),
        P(("blk", "tensor"), None),
        P(("blk", "tensor"), None),
    )
    return jax.shard_map(
        functools.partial(per_device, mesh.shape["blk"], mesh.shape["tensor"]),
        mesh=mesh,
        in_specs=placed,
        out_specs=P(("blk", "tensor"), None),
        check_vma=False,
    )
```

```python
import functools

import jax
import jax.numpy as jnp
from jax import lax
from jax.experimental import pallas as pl
from jax.experimental.pallas import tpu as pltpu
from jax.sharding import PartitionSpec as P

MESH = pl.DeviceIdType.MESH
CHUNKS = 4
TILE = 512


def kernel(
    outers, inners, tensors,
    tok, wg, wu, wd, out,
    wgv, wuv, wdv, gathered, x2d, gacc, uacc, hid, own, part, near, stage, mid, held, far,
    tok_sem, w_sem, ag_send, ag_recv, in_send, in_recv, fw_send, fw_recv,
    near_send, near_recv, mid_send, mid_recv, far_send, far_recv,
):
    blk, ten = lax.axis_index("blk"), lax.axis_index("tensor")
    core, chip = lax.rem(blk, 2), lax.div(blk, 2)
    outer, inner = lax.div(chip, inners), lax.rem(chip, inners)
    other = 1 - core
    mate = (blk + 1 - 2 * core, ten)
    planes = inners * tensors
    plane = inner * tensors + ten
    width = tok.shape[1] // CHUNKS
    rows = tok.shape[0]
    share = rows // tensors

    def outer_peer(step):
        to = lax.rem(outer + step, outers)
        return to, ((to * inners + inner) * 2 + core, ten)

    def inner_peer(step):
        to = lax.rem(inner + step, inners)
        return to, ((outer * inners + to) * 2 + core, ten)

    def plane_peer(step):
        to = lax.rem(plane + step, planes)
        return to, ((outer * inners + lax.div(to, tensors)) * 2 + core, lax.rem(to, tensors))

    def cols(k):
        return pl.ds(k * width, width)

    def tok_copy(k):
        return pltpu.make_async_copy(tok.at[:, cols(k)], gathered.at[k, core, inner, outer], tok_sem.at[k])

    def w_copy(which, k):
        src, dst = ((wg, wgv), (wu, wuv), (wd, wdv))[which]
        return pltpu.make_async_copy(src.at[:, cols(k)], dst.at[k], w_sem.at[which, k])

    for k in range(CHUNKS):
        tok_copy(k).start()
    for k in range(CHUNKS):
        w_copy(0, k).start()
        w_copy(1, k).start()

    barrier = pltpu.get_barrier_semaphore()
    pl.semaphore_signal(barrier, inc=1, device_id=mate, device_id_type=MESH)

    for step in range(1, planes):
        pl.semaphore_signal(barrier, inc=1, device_id=plane_peer(step)[1], device_id_type=MESH)
    for step in range(1, outers):
        pl.semaphore_signal(barrier, inc=1, device_id=outer_peer(step)[1], device_id_type=MESH)
    pl.semaphore_wait(barrier, planes + outers - 1)

    def ag_copy(k, step, slot):
        to, device = outer_peer(step)
        block = gathered.at[k, core, inner, slot]
        return pltpu.make_async_remote_copy(
            src_ref=block, dst_ref=block,
            send_sem=ag_send.at[k, to], recv_sem=ag_recv.at[k, slot],
            device_id=device, device_id_type=MESH,
        )

    def in_copy(k, step, slot):
        to, device = inner_peer(step)
        block = gathered.at[k, core, slot]
        return pltpu.make_async_remote_copy(
            src_ref=block, dst_ref=block,
            send_sem=in_send.at[k, to], recv_sem=in_recv.at[k, slot],
            device_id=device, device_id_type=MESH,
        )

    def fw_copy(k, side, slot):
        block = gathered.at[k, side, slot]
        return pltpu.make_async_remote_copy(
            src_ref=block, dst_ref=block,
            send_sem=fw_send.at[k, slot], recv_sem=fw_recv.at[k, slot],
            device_id=mate, device_id_type=MESH,
        )

    for k in range(CHUNKS):
        tok_copy(k).wait()

        for step in range(1, outers):
            ag_copy(k, step, outer).start()

    for k in range(CHUNKS):
        w_copy(2, k).start()

    def forward(k):
        for step in range(1, outers):
            ag_copy(k, step, outer_peer(step)[0]).wait_recv()
        for step in range(1, inners):
            in_copy(k, step, inner).start()
        fw_copy(k, core, inner).start()

    def hand_over(k):
        for step in range(1, inners):
            slot = inner_peer(step)[0]
            in_copy(k, step, slot).wait_recv()
            fw_copy(k, core, slot).start()

    gacc[...] = jnp.zeros_like(gacc)
    uacc[...] = jnp.zeros_like(uacc)

    def project(k, start, stop):
        @pl.loop(start, stop)
        def _(step):
            at = pl.ds(pl.multiple_of(step * TILE, TILE), TILE)
            for side in range(2):
                for i in range(inners):
                    for o in range(outers):
                        low = ((side * inners + i) * outers + o) * rows
                        x2d[low:low + rows, :] = gathered[k, side, i, o, :, at]
            x = x2d[...]
            dims = (((1,), (1,)), ((), ()))
            gacc[...] += lax.dot_general(x, wgv[k, :, at], dims, preferred_element_type=jnp.float32)
            uacc[...] += lax.dot_general(x, wuv[k, :, at], dims, preferred_element_type=jnp.float32)

    tiles = width // TILE
    forward(0)
    for k in range(CHUNKS):
        if k + 1 < CHUNKS and k:
            forward(k + 1)
        if not k:
            hand_over(0)
            forward(1)
        for i in range(inners):
            fw_copy(k, other, i).wait_recv()
        w_copy(0, k).wait()
        w_copy(1, k).wait()
        project(k, 0, tiles // 2)
        if k + 1 < CHUNKS:
            hand_over(k + 1)
        project(k, tiles // 2, tiles)

    gate = gacc[...]
    hid[...] = (gate / (1.0 + jnp.exp(-gate)) * uacc[...]).astype(hid.dtype)

    def near_copy(j):
        return pltpu.make_async_remote_copy(
            src_ref=part.at[j, other], dst_ref=near.at[j],
            send_sem=near_send.at[j], recv_sem=near_recv.at[j],
            device_id=mate, device_id_type=MESH,
        )

    def mid_copy(j, step, slot):
        to, device = plane_peer(step)
        return pltpu.make_async_remote_copy(
            src_ref=stage.at[j, to], dst_ref=mid.at[j, slot],
            send_sem=mid_send.at[j, to], recv_sem=mid_recv.at[j, slot],
            device_id=device, device_id_type=MESH,
        )

    def far_copy(j, step, slot):
        to, device = outer_peer(step)
        return pltpu.make_async_remote_copy(
            src_ref=held.at[j, to], dst_ref=far.at[j, slot],
            send_sem=far_send.at[j, to], recv_sem=far_recv.at[j, slot],
            device_id=device, device_id_type=MESH,
        )

    half = inners * outers * rows

    def down(j):
        w_copy(2, j).wait()

        @pl.loop(0, tiles)
        def _(step):
            at = pl.ds(pl.multiple_of(step * TILE, TILE), TILE)
            p = jnp.dot(hid[...], wdv[j, :, at], preferred_element_type=jnp.float32)
            for side in range(2):
                piece = p[side * half:(side + 1) * half]
                own[j, side, :, at] = piece
                part[j, side, :, at] = piece.astype(part.dtype)

        near_copy(j).start()

    def send_mid(j):
        near_copy(j).wait_recv()

        @pl.loop(0, tiles)
        def _(step):
            at = pl.ds(pl.multiple_of(step * TILE, TILE), TILE)
            s = own[j, core, :, at] + near[j, :, at].astype(jnp.float32)
            for i in range(inners):
                for o in range(outers):
                    for t in range(tensors):
                        low = ((i * outers + o) * tensors + t) * share
                        stage[j, i * tensors + t, o, :, at] = s[low:low + share].astype(stage.dtype)

        for step in range(1, planes):
            mid_copy(j, step, plane).start()

    def send_far(j):
        for step in range(1, planes):
            mid_copy(j, step, plane_peer(step)[0]).wait_recv()
        for o in range(outers):
            total = stage[j, plane, o].astype(jnp.float32)
            for step in range(1, planes):
                total += mid[j, plane_peer(step)[0], o].astype(jnp.float32)
            held[j, o] = total.astype(held.dtype)
        for step in range(1, outers):
            far_copy(j, step, outer).start()

    def finish(j):
        total = held[j, outer].astype(jnp.float32)
        for step in range(1, outers):
            slot = outer_peer(step)[0]
            far_copy(j, step, slot).wait_recv()
            total += far[j, slot].astype(jnp.float32)
        out[:, j * width:(j + 1) * width] = total.astype(out.dtype)

    for j in range(CHUNKS):
        down(j)
        if j:
            send_mid(j - 1)
    send_mid(CHUNKS - 1)
    for j in range(CHUNKS):
        send_far(j)
    for j in range(CHUNKS):
        finish(j)

    for k in range(CHUNKS):
        for step in range(1, outers):
            ag_copy(k, step, outer).wait_send()
            far_copy(k, step, outer).wait_send()
        for step in range(1, inners):
            in_copy(k, step, inner).wait_send()
        for step in range(1, planes):
            mid_copy(k, step, plane).wait_send()
        for i in range(inners):
            fw_copy(k, core, i).wait_send()
        near_copy(k).wait_send()


def per_device(blks, tensors, tokens, gate_weight, up_weight, down_weight):
    rows, depth = tokens.shape
    units = gate_weight.shape[0]
    chips, width = blks // 2, depth // CHUNKS
    inners = 2 if chips % 2 == 0 else 1
    outers, planes, share = chips // inners, inners * tensors, rows // tensors
    everyone, half = blks * rows, chips * rows
    bf, f32, dma = jnp.bfloat16, jnp.float32, pltpu.SemaphoreType.DMA
    anywhere = pl.BlockSpec(memory_space=pl.ANY)
    return pl.pallas_call(
        functools.partial(kernel, outers, inners, tensors),
        out_shape=jax.ShapeDtypeStruct((share, depth), bf),
        in_specs=[anywhere] * 4,
        out_specs=pl.BlockSpec(memory_space=pltpu.VMEM),
        scratch_shapes=[
            pltpu.VMEM((CHUNKS, units, width), bf),
            pltpu.VMEM((CHUNKS, units, width), bf),
            pltpu.VMEM((CHUNKS, units, width), bf),
            pltpu.VMEM((CHUNKS, 2, inners, outers, rows, width), bf),
            pltpu.VMEM((everyone, TILE), bf),
            pltpu.VMEM((everyone, units), f32),
            pltpu.VMEM((everyone, units), f32),
            pltpu.VMEM((everyone, units), bf),
            pltpu.VMEM((CHUNKS, 2, half, width), f32),
            pltpu.VMEM((CHUNKS, 2, half, width), bf),
            pltpu.VMEM((CHUNKS, half, width), bf),
            pltpu.VMEM((CHUNKS, planes, outers, share, width), bf),
            pltpu.VMEM((CHUNKS, planes, outers, share, width), bf),
            pltpu.VMEM((CHUNKS, outers, share, width), bf),
            pltpu.VMEM((CHUNKS, outers, share, width), bf),
            dma((CHUNKS,)),
            dma((3, CHUNKS)),
            dma((CHUNKS, outers)),
            dma((CHUNKS, outers)),
            dma((CHUNKS, inners)),
            dma((CHUNKS, inners)),
            dma((CHUNKS, inners)),
            dma((CHUNKS, inners)),
            dma((CHUNKS,)),
            dma((CHUNKS,)),
            dma((CHUNKS, planes)),
            dma((CHUNKS, planes)),
            dma((CHUNKS, outers)),
            dma((CHUNKS, outers)),
        ],
        compiler_params=pltpu.CompilerParams(
            collective_id=0, has_side_effects=True, vmem_limit_bytes=60 * 1024 * 1024
        ),
    )(tokens, gate_weight, up_weight, down_weight)


def solution(mesh):
    placed = (
        P("blk", None),
        P(("blk", "tensor"), None),
        P(("blk", "tensor"), None),
        P(("blk", "tensor"), None),
    )
    return jax.shard_map(
        functools.partial(per_device, mesh.shape["blk"], mesh.shape["tensor"]),
        mesh=mesh,
        in_specs=placed,
        out_specs=P(("blk", "tensor"), None),
        check_vma=False,
    )
```

```python
import functools

import jax
import jax.numpy as jnp
from jax import lax
from jax.experimental import pallas as pl
from jax.experimental.pallas import tpu as pltpu
from jax.sharding import PartitionSpec as P

MESH = pl.DeviceIdType.MESH
CHUNKS = 4
TILE = 512


def kernel(
    outers, inners, tensors,
    tok, wg, wu, wd, out,
    wgv, wuv, wdv, gathered, x2d, gacc, uacc, hid, own, part, near, stage, mid, held, far,
    tok_sem, w_sem, ag_send, ag_recv, in_send, in_recv, fw_send, fw_recv,
    near_send, near_recv, mid_send, mid_recv, far_send, far_recv,
):
    blk, ten = lax.axis_index("blk"), lax.axis_index("tensor")
    core, chip = lax.rem(blk, 2), lax.div(blk, 2)
    outer, inner = lax.div(chip, inners), lax.rem(chip, inners)
    other = 1 - core
    mate = (blk + 1 - 2 * core, ten)
    planes = inners * tensors
    plane = inner * tensors + ten
    width = tok.shape[1] // CHUNKS
    rows = tok.shape[0]
    share = rows // tensors

    def outer_peer(step):
        to = lax.rem(outer + step, outers)
        return to, ((to * inners + inner) * 2 + core, ten)

    def inner_peer(step):
        to = lax.rem(inner + step, inners)
        return to, ((outer * inners + to) * 2 + core, ten)

    def plane_peer(step):
        to = lax.rem(plane + step, planes)
        return to, ((outer * inners + lax.div(to, tensors)) * 2 + core, lax.rem(to, tensors))

    def cols(k):
        return pl.ds(k * width, width)

    def tok_copy(k):
        return pltpu.make_async_copy(tok.at[:, cols(k)], gathered.at[k, core, inner, outer], tok_sem.at[k])

    def w_copy(which, k):
        src, dst = ((wg, wgv), (wu, wuv), (wd, wdv))[which]
        return pltpu.make_async_copy(src.at[:, cols(k)], dst.at[k], w_sem.at[which, k])

    for k in range(CHUNKS):
        tok_copy(k).start()
    for k in range(CHUNKS):
        w_copy(0, k).start()
        w_copy(1, k).start()

    barrier = pltpu.get_barrier_semaphore()
    pl.semaphore_signal(barrier, inc=1, device_id=mate, device_id_type=MESH)

    for step in range(1, planes):
        pl.semaphore_signal(barrier, inc=1, device_id=plane_peer(step)[1], device_id_type=MESH)
    for step in range(1, outers):
        pl.semaphore_signal(barrier, inc=1, device_id=outer_peer(step)[1], device_id_type=MESH)
    pl.semaphore_wait(barrier, planes + outers - 1)

    def ag_copy(k, step, slot):
        to, device = outer_peer(step)
        block = gathered.at[k, core, inner, slot]
        return pltpu.make_async_remote_copy(
            src_ref=block, dst_ref=block,
            send_sem=ag_send.at[k, to], recv_sem=ag_recv.at[k, slot],
            device_id=device, device_id_type=MESH,
        )

    def in_copy(k, step, slot):
        to, device = inner_peer(step)
        block = gathered.at[k, core, slot]
        return pltpu.make_async_remote_copy(
            src_ref=block, dst_ref=block,
            send_sem=in_send.at[k, to], recv_sem=in_recv.at[k, slot],
            device_id=device, device_id_type=MESH,
        )

    def fw_copy(k, side, slot):
        block = gathered.at[k, side, slot]
        return pltpu.make_async_remote_copy(
            src_ref=block, dst_ref=block,
            send_sem=fw_send.at[k, slot], recv_sem=fw_recv.at[k, slot],
            device_id=mate, device_id_type=MESH,
        )

    for k in range(CHUNKS):
        tok_copy(k).wait()

        for step in range(1, outers):
            ag_copy(k, step, outer).start()

    for k in range(CHUNKS):
        w_copy(2, k).start()

    def forward(k):
        for step in range(1, outers):
            ag_copy(k, step, outer_peer(step)[0]).wait_recv()
        for step in range(1, inners):
            in_copy(k, step, inner).start()
        fw_copy(k, core, inner).start()

    def hand_over(k):
        for step in range(1, inners):
            slot = inner_peer(step)[0]
            in_copy(k, step, slot).wait_recv()
            fw_copy(k, core, slot).start()

    gacc[...] = jnp.zeros_like(gacc)
    uacc[...] = jnp.zeros_like(uacc)

    def collect(k):
        for i in range(inners):
            fw_copy(k, other, i).wait_recv()
        for side in range(2):
            for i in range(inners):
                for o in range(outers):
                    low = ((side * inners + i) * outers + o) * rows
                    x2d[low:low + rows, :] = gathered[k, side, i, o]
        w_copy(0, k).wait()
        w_copy(1, k).wait()

    def project(k, weight, acc):
        acc[...] += lax.dot_general(
            weight[k], x2d[...], (((1,), (1,)), ((), ())), preferred_element_type=jnp.float32
        )

    tiles = width // TILE
    forward(0)
    forward(1)
    hand_over(0)
    forward(2)
    for k in range(CHUNKS):
        collect(k)
        project(k, wgv, gacc)
        if k == 0:
            for later in range(3, CHUNKS):
                forward(later)
        if k + 1 < CHUNKS:
            hand_over(k + 1)
        project(k, wuv, uacc)

    gate = gacc[...]
    hid[...] = (gate / (1.0 + jnp.exp(-gate)) * uacc[...]).T.astype(hid.dtype)

    def near_copy(j):
        return pltpu.make_async_remote_copy(
            src_ref=part.at[j, other], dst_ref=near.at[j],
            send_sem=near_send.at[j], recv_sem=near_recv.at[j],
            device_id=mate, device_id_type=MESH,
        )

    def mid_copy(j, step, slot):
        to, device = plane_peer(step)
        return pltpu.make_async_remote_copy(
            src_ref=stage.at[j, to], dst_ref=mid.at[j, slot],
            send_sem=mid_send.at[j, to], recv_sem=mid_recv.at[j, slot],
            device_id=device, device_id_type=MESH,
        )

    def far_copy(j, step, slot):
        to, device = outer_peer(step)
        return pltpu.make_async_remote_copy(
            src_ref=held.at[j, to], dst_ref=far.at[j, slot],
            send_sem=far_send.at[j, to], recv_sem=far_recv.at[j, slot],
            device_id=device, device_id_type=MESH,
        )

    half = inners * outers * rows

    def down(j):
        w_copy(2, j).wait()

        @pl.loop(0, tiles)
        def _(step):
            at = pl.ds(pl.multiple_of(step * TILE, TILE), TILE)
            p = jnp.dot(hid[...], wdv[j, :, at], preferred_element_type=jnp.float32)
            for side in range(2):
                piece = p[side * half:(side + 1) * half]
                own[j, side, :, at] = piece
                part[j, side, :, at] = piece.astype(part.dtype)

        near_copy(j).start()

    def send_mid(j):
        near_copy(j).wait_recv()

        @pl.loop(0, tiles)
        def _(step):
            at = pl.ds(pl.multiple_of(step * TILE, TILE), TILE)
            s = own[j, core, :, at] + near[j, :, at].astype(jnp.float32)
            for i in range(inners):
                for o in range(outers):
                    for t in range(tensors):
                        low = ((i * outers + o) * tensors + t) * share
                        stage[j, i * tensors + t, o, :, at] = s[low:low + share].astype(stage.dtype)

        for step in range(1, planes):
            mid_copy(j, step, plane).start()

    def send_far(j):
        for step in range(1, planes):
            mid_copy(j, step, plane_peer(step)[0]).wait_recv()
        for o in range(outers):
            total = stage[j, plane, o].astype(jnp.float32)
            for step in range(1, planes):
                total += mid[j, plane_peer(step)[0], o].astype(jnp.float32)
            held[j, o] = total.astype(held.dtype)
        for step in range(1, outers):
            far_copy(j, step, outer).start()

    def finish(j):
        total = held[j, outer].astype(jnp.float32)
        for step in range(1, outers):
            slot = outer_peer(step)[0]
            far_copy(j, step, slot).wait_recv()
            total += far[j, slot].astype(jnp.float32)
        out[:, j * width:(j + 1) * width] = total.astype(out.dtype)

    for j in range(CHUNKS):
        down(j)
        if j:
            send_mid(j - 1)
    send_far(0)
    send_mid(CHUNKS - 1)
    for j in range(1, CHUNKS):
        send_far(j)
        finish(j - 1)
    finish(CHUNKS - 1)

    for k in range(CHUNKS):
        for step in range(1, outers):
            ag_copy(k, step, outer).wait_send()
            far_copy(k, step, outer).wait_send()
        for step in range(1, inners):
            in_copy(k, step, inner).wait_send()
        for step in range(1, planes):
            mid_copy(k, step, plane).wait_send()
        for i in range(inners):
            fw_copy(k, core, i).wait_send()
        near_copy(k).wait_send()


def per_device(blks, tensors, tokens, gate_weight, up_weight, down_weight):
    rows, depth = tokens.shape
    units = gate_weight.shape[0]
    chips, width = blks // 2, depth // CHUNKS
    inners = 2 if chips % 2 == 0 else 1
    outers, planes, share = chips // inners, inners * tensors, rows // tensors
    everyone, half = blks * rows, chips * rows
    bf, f32, dma = jnp.bfloat16, jnp.float32, pltpu.SemaphoreType.DMA
    anywhere = pl.BlockSpec(memory_space=pl.ANY)
    return pl.pallas_call(
        functools.partial(kernel, outers, inners, tensors),
        out_shape=jax.ShapeDtypeStruct((share, depth), bf),
        in_specs=[anywhere] * 4,
        out_specs=pl.BlockSpec(memory_space=pltpu.VMEM),
        scratch_shapes=[
            pltpu.VMEM((CHUNKS, units, width), bf),
            pltpu.VMEM((CHUNKS, units, width), bf),
            pltpu.VMEM((CHUNKS, units, width), bf),
            pltpu.VMEM((CHUNKS, 2, inners, outers, rows, width), bf),
            pltpu.VMEM((everyone, width), bf),
            pltpu.VMEM((units, everyone), f32),
            pltpu.VMEM((units, everyone), f32),
            pltpu.VMEM((everyone, units), bf),
            pltpu.VMEM((CHUNKS, 2, half, width), f32),
            pltpu.VMEM((CHUNKS, 2, half, width), bf),
            pltpu.VMEM((CHUNKS, half, width), bf),
            pltpu.VMEM((CHUNKS, planes, outers, share, width), bf),
            pltpu.VMEM((CHUNKS, planes, outers, share, width), bf),
            pltpu.VMEM((CHUNKS, outers, share, width), bf),
            pltpu.VMEM((CHUNKS, outers, share, width), bf),
            dma((CHUNKS,)),
            dma((3, CHUNKS)),
            dma((CHUNKS, outers)),
            dma((CHUNKS, outers)),
            dma((CHUNKS, inners)),
            dma((CHUNKS, inners)),
            dma((CHUNKS, inners)),
            dma((CHUNKS, inners)),
            dma((CHUNKS,)),
            dma((CHUNKS,)),
            dma((CHUNKS, planes)),
            dma((CHUNKS, planes)),
            dma((CHUNKS, outers)),
            dma((CHUNKS, outers)),
        ],
        compiler_params=pltpu.CompilerParams(
            collective_id=0, has_side_effects=True, vmem_limit_bytes=60 * 1024 * 1024
        ),
    )(tokens, gate_weight, up_weight, down_weight)


def solution(mesh):
    placed = (
        P("blk", None),
        P(("blk", "tensor"), None),
        P(("blk", "tensor"), None),
        P(("blk", "tensor"), None),
    )
    return jax.shard_map(
        functools.partial(per_device, mesh.shape["blk"], mesh.shape["tensor"]),
        mesh=mesh,
        in_specs=placed,
        out_specs=P(("blk", "tensor"), None),
        check_vma=False,
    )
```
